32 devices in a mesh: patch: 8 (over z, y), sub: 4 (over x, core).
Axes of the slice: x: 2, y: 2, z: 4, core: 2. Of those that a mesh axis runs over, the one named last changes fastest.
Arguments:
- sources: int32 [128, 2], replicated, may hold values from 0 to 16383
- diag_coef: float32 [16384], P(('patch', 'sub')), may hold values from 1 to 2
- tiles: float32 [128, 6, 128, 128], P(('patch', 'sub')), may hold values from -0.109375 to 0.109375
- tile_cols: int32 [128, 6], P(('patch', 'sub')), may hold values from 0 to 7
- send_rows: int32 [32, 4, 128], P(('patch', 'sub')), may hold values from 0 to 511
- recv_rows: int32 [32, 512], P(('patch', 'sub')), may hold values from 0 to 511, each once within a row
- bounds: float32 [2], replicated, may hold values from 0.3 to 3.2, as said below
Outputs:
- solution: float32 [16384, 128], P(('patch', 'sub'))
- res_norm: float32 [128], replicated
The draws below stay inside these ranges and needn't reach their ends.
Inputs may be any that keep to these rules, and one draw needn't show every extreme that they name: bounds[0] lies in 0.3 to 0.5 and bounds[1] in 2.6 to 3.2.
All inputs are finite; a program needn't handle non-finite values.
Results may differ from the reference program's by a relative error of at most 0.0001.
Values sent between devices are 32-bit elements; how exact they have to be, the bound alone decides.
A program may use at most 64 MiB of HBM per device.

```python
import jax
import jax.numpy as jnp
from jax import lax

BLOCK = 128
BLK_DEV = 4
NB = 6
K = 128
S = 128
ITERS = 8
V_DEV = 512
VERTS = 16384
BLOCKS = 128
H = 512
HB = 4
NSRC = 2
N_PATCH = 8
N_SUB = 4
DEVICES = 32


def draw_bounds(key, part):
    first_key, second_key = jax.random.split(key)
    lower_end = jax.random.uniform(first_key, (), jnp.float32, 0.3, 0.5)
    upper_end = jax.random.uniform(second_key, (), jnp.float32, 2.6, 3.2)
    return jnp.stack([lower_end, upper_end]).astype(jnp.float32)


def with_ends(drawn, own_key, smallest, largest):
    longest = drawn.shape.index(max(drawn.shape))
    spots = []
    for shift in (0, 1):
        where = [jax.random.randint(jax.random.fold_in(own_key, axis), (), 0, length) for axis, length in enumerate(drawn.shape)]
        where[longest] = (where[longest] + shift) % drawn.shape[longest]
        spots.append(tuple(where))
    return drawn.at[spots[0]].set(smallest).at[spots[1]].set(largest)


def block_scale(rng, extent, cuts, low, high):
    def one(position, shards_of):
        draws = jax.random.uniform(jax.random.fold_in(jax.random.fold_in(rng, 6), position), (shards_of,), jnp.float32, low / len(cuts), high / len(cuts))
        return jnp.repeat(jnp.exp(draws), extent[position] // shards_of).reshape((-1,) + (1,) * (len(extent) - position - 1))

    level = one(*cuts[0])
    for cut in cuts[1:]:
        level = level * one(*cut)
    return level


def noise(key, dims, width, most, pieces=(), held_as=jnp.bfloat16):
    values = width * jax.random.normal(key, dims, jnp.float32)
    if pieces:
        values = values * block_scale(key, dims, pieces, -0.22, 0.18)
    return jnp.clip(values, -most, most).astype(held_as)


def setup_inputs(seed: int = 0) -> dict:
    keys = jax.random.split(jax.random.key(seed), 8)
    sources = with_ends(jax.random.randint(keys[0], (K, NSRC), 0, VERTS), jax.random.fold_in(keys[0], 1), 0, VERTS - 1).astype(jnp.int32)
    diag_coef = jnp.clip(1.0 + 1.0 * jax.random.uniform(keys[1], (VERTS,), jnp.float32) ** block_scale(keys[1], (VERTS,), ((0, 32),), -0.2, 0.2), 1.0, 2.0)
    tiles = noise(keys[2], (BLOCKS, NB, BLOCK, BLOCK), (4 * NB * BLOCK) ** -0.5, 0.109375, ((0, 32),), jnp.float32)
    tile_cols = with_ends(jax.random.randint(keys[3], (BLOCKS, NB), 0, BLK_DEV + HB), jax.random.fold_in(keys[3], 1), 0, (BLK_DEV + HB) - 1).astype(jnp.int32)
    send_rows = with_ends(jax.random.randint(keys[4], (DEVICES, 4, S), 0, V_DEV), jax.random.fold_in(keys[4], 1), 0, V_DEV - 1).astype(jnp.int32)
    recv_rows = jax.vmap(lambda own: jax.random.permutation(own, H))(jax.random.split(keys[5], DEVICES)).reshape((DEVICES, H)).astype(jnp.int32)
    bounds = draw_bounds(jax.random.fold_in(keys[7], 71), 0)
    return dict(sources=sources, diag_coef=diag_coef, tiles=tiles, tile_cols=tile_cols, send_rows=send_rows, recv_rows=recv_rows, bounds=bounds)


def build_right(sources, total_rows):
    columns = sources.shape[0]
    which = jnp.arange(columns, dtype=jnp.int32)[:, None]
    flat_index = (sources * columns + which).reshape(-1)
    counts = jax.ops.segment_sum(jnp.ones(flat_index.shape, jnp.float32), flat_index, num_segments=total_rows * columns)
    return counts.reshape(total_rows, columns)

def pick_rows(values, index):
    return values[index]

def operate(field, diag_coef, tiles, tile_cols, send_rows, recv_rows):
    devices = N_PATCH * N_SUB
    rows = BLK_DEV * BLOCK
    columns = field.shape[1]
    local = field.reshape(devices, rows, columns)
    packed = jax.vmap(pick_rows)(local, send_rows)
    packed = packed.reshape(N_PATCH, N_SUB, 4, S, columns)
    below_patch = jnp.roll(packed[:, :, 1], 1, axis=0)
    above_patch = jnp.roll(packed[:, :, 0], -1, axis=0)
    below_sub = jnp.roll(packed[:, :, 3], 1, axis=1)
    above_sub = jnp.roll(packed[:, :, 2], -1, axis=1)
    received = jnp.concatenate([below_patch, above_patch, below_sub, above_sub], axis=2)
    received = received.reshape(devices, 4 * S, columns)
    halo_rows = jax.vmap(pick_rows)(received, recv_rows)
    extended = jnp.concatenate([local, halo_rows], axis=1).reshape(devices, BLK_DEV + HB, BLOCK, columns)
    tile_blocks = tiles.reshape(devices, BLK_DEV, NB, BLOCK, BLOCK)
    col_blocks = tile_cols.reshape(devices, BLK_DEV, NB)

    def device_product(inputs):
        dev_tiles, dev_cols, dev_ext = inputs
        summed = jnp.zeros((BLK_DEV, BLOCK, columns), jnp.float32)
        for slot_index in range(NB):
            summed = summed + jnp.einsum('bij,bjk->bik', dev_tiles[:, slot_index], dev_ext[dev_cols[:, slot_index]], precision=lax.Precision.HIGHEST)
        return summed
    coupled = lax.map(device_product, (tile_blocks, col_blocks, extended)).reshape(devices * rows, columns)
    return diag_coef[:, None] * field + coupled

def reference(sources, diag_coef, tiles, tile_cols, send_rows, recv_rows, bounds):
    right_side = build_right(sources, VERTS)
    centre = (bounds[0] + bounds[1]) / 2.0
    half_width = (bounds[1] - bounds[0]) / 2.0
    ratio = centre / half_width
    damping = 1.0 / ratio
    solution = jnp.zeros_like(right_side)
    residual = right_side
    direction = right_side / centre
    for iteration in range(ITERS):
        solution = solution + direction
        residual = residual - operate(direction, diag_coef, tiles, tile_cols, send_rows, recv_rows)
        if iteration + 1 < ITERS:
            damping_next = 1.0 / (2.0 * ratio - damping)
            direction = damping_next * damping * direction + 2.0 * damping_next / half_width * residual
            damping = damping_next
    final = right_side - operate(solution, diag_coef, tiles, tile_cols, send_rows, recv_rows)
    res_norm = jnp.sqrt(lax.optimization_barrier(jnp.sum(final * final, axis=0)))
    return (solution, res_norm)
```

```python
import functools

import jax
import jax.numpy as jnp
from jax import lax
from jax.experimental import pallas as pl
from jax.experimental.pallas import tpu as pltpu
from jax.sharding import PartitionSpec as P

ITERS = 8
MESH = pl.DeviceIdType.MESH
F32 = jnp.float32
BF16 = jnp.bfloat16


def halves(value):
    high = value.astype(BF16)
    return high, (value - high.astype(F32)).astype(BF16)


def product(high, low, pair, columns):
    wide = jnp.dot(high, pair, preferred_element_type=F32)
    narrow = jnp.dot(low, pair[:, :columns], preferred_element_type=F32)
    return wide[:, :columns] + wide[:, columns:] + narrow


def kernel(
    n_patch, n_sub,
    sources_ref, diag_ref, tiles_hbm, cols_ref, sends_ref, receives_ref, bounds_ref,
    solution_ref, norm_ref,
    tiles_ref, near_hi, near_lo, far_hi, far_lo, halo_hi, halo_lo,
    direction_ref, residual_ref, packed_residual, total_ref, pair_ref, heard_pair,
    packed_ref, heard_ref, heard_rows, norms_ref,
    tile_sems, row_send, row_recv, send_sems, recv_sems, norm_send, norm_recv,
):
    blk_rows, per_row, size, _ = tiles_hbm.shape
    rows = blk_rows * size
    n_src, columns = sources_ref.shape
    sent = sends_ref.shape[2]
    halo = receives_ref.shape[1]
    packed_rows = 4 * sent
    patch, sub = lax.axis_index("patch"), lax.axis_index("sub")
    devices = n_patch * n_sub
    me = patch * n_sub + sub

    copies = [
        pltpu.make_async_copy(tiles_hbm.at[b], tiles_ref.at[b], tile_sems.at[b])
        for b in range(blk_rows)
    ]
    for copy in copies:
        copy.start()

    barrier = pltpu.get_barrier_semaphore()

    @pl.loop(1, devices)
    def _(step):
        other = lax.rem(me + step, devices)
        pl.semaphore_signal(
            barrier, inc=1, device_id=(other // n_sub, lax.rem(other, n_sub)), device_id_type=MESH
        )

    lower_patch = lax.rem(patch + n_patch - 1, n_patch)
    upper_patch = lax.rem(patch + 1, n_patch)
    lower_sub = lax.rem(sub + n_sub - 1, n_sub)
    upper_sub = lax.rem(sub + 1, n_sub)
    targets = [(lower_patch, sub), (upper_patch, sub), (patch, lower_sub), (patch, upper_sub)]
    lands = [1, 0, 3, 2]
    origins = [targets[0], targets[1], targets[2], targets[3]]

    low_end = jnp.full((1, columns), bounds_ref[0], F32)
    high_end = jnp.full((1, columns), bounds_ref[1], F32)
    centre = (low_end + high_end) / 2.0
    half_width = (high_end - low_end) / 2.0
    ratio = centre / half_width

    def counted(ids):
        total = jnp.zeros(ids.shape, F32)
        for s in range(n_src):
            total = total + jnp.where(sources_ref[s : s + 1, :] == ids, 1.0, 0.0)
        return total

    right_side = counted(me * rows + lax.broadcasted_iota(jnp.int32, (rows, columns), 0))
    direction = right_side / centre
    residual_ref[...] = right_side
    direction_ref[...] = direction
    solution_ref[...] = direction
    high, low = halves(direction)
    pair_ref[:, :columns] = high
    pair_ref[:, columns:] = low

    def as_column(row, width):
        return jnp.broadcast_to(row, (width, row.shape[1])).T

    picks = []
    for j in range(4):
        column = as_column(sends_ref[j], columns)
        mine = counted(me * rows + column)
        packed_residual[pl.ds(j * sent, sent)] = mine
        packed_ref[0, j] = mine / centre
        wide = as_column(sends_ref[j], rows)
        picks.append(
            jnp.where(wide == lax.broadcasted_iota(jnp.int32, (sent, rows), 1), 1.0, 0.0).astype(BF16)
        )
    pick = jnp.concatenate(picks, axis=0)
    place = jnp.where(
        receives_ref[...] == lax.broadcasted_iota(jnp.int32, (packed_rows, halo), 0), 1.0, 0.0
    ).astype(BF16)

    pl.semaphore_wait(barrier, devices - 1)
    row_copies = []
    for j in range(4):
        copy = pltpu.make_async_remote_copy(
            src_ref=sends_ref.at[j], dst_ref=heard_rows.at[lands[j]],
            send_sem=row_send.at[j], recv_sem=row_recv.at[lands[j]],
            device_id=targets[j], device_id_type=MESH,
        )
        copy.start()
        row_copies.append(copy)

    eye = lax.broadcasted_iota(jnp.int32, (size, size), 0) == lax.broadcasted_iota(
        jnp.int32, (size, size), 1
    )
    for b in range(blk_rows):
        copies[b].wait()
        for c in range(blk_rows + halo // size):
            block = jnp.zeros((size, size), F32)
            for n in range(per_row):
                block = block + tiles_ref[b, n] * (cols_ref[b, n] == c).astype(F32)
            if c == b:
                block = block + jnp.where(eye, diag_ref[b : b + 1, :], 0.0)
            high, low = halves(block)
            at = pl.ds(packed_rows + b * size, size)
            if c < blk_rows:
                near_hi[at, pl.ds(c * size, size)] = high
                near_lo[at, pl.ds(c * size, size)] = low
            else:
                place_at = pl.ds((c - blk_rows) * size, size)
                halo_hi[pl.ds(b * size, size), place_at] = high
                halo_lo[pl.ds(b * size, size), place_at] = low
    own = pl.ds(packed_rows, rows)
    first = pl.ds(0, packed_rows)
    for halo_part, far, near in ((halo_hi, far_hi, near_hi), (halo_lo, far_lo, near_lo)):
        far[own] = lax.dot_general(
            halo_part[...], place, (((1,), (1,)), ((), ())), preferred_element_type=F32
        ).astype(BF16)
        far[first] = jnp.dot(pick, far[own], preferred_element_type=F32).astype(BF16)
        near[first] = jnp.dot(pick, near[own], preferred_element_type=F32).astype(BF16)

    for j in range(4):
        row_copies[j].wait()
    for j in range(4):
        base = (origins[j][0] * n_sub + origins[j][1]) * rows
        value = counted(base + as_column(heard_rows[j], columns)) / centre
        high, low = halves(value)
        heard_pair[pl.ds(j * sent, sent), :columns] = high
        heard_pair[pl.ds(j * sent, sent), columns:] = low

    def exchange(slot, j):
        return pltpu.make_async_remote_copy(
            src_ref=packed_ref.at[slot, j], dst_ref=heard_ref.at[slot, lands[j]],
            send_sem=send_sems.at[slot, j], recv_sem=recv_sems.at[slot, lands[j]],
            device_id=targets[j], device_id_type=MESH,
        )

    def arrival(slot, j):
        return pltpu.make_async_remote_copy(
            src_ref=packed_ref.at[slot, j], dst_ref=heard_ref.at[slot, j],
            send_sem=send_sems.at[slot, j], recv_sem=recv_sems.at[slot, j],
            device_id=targets[j], device_id_type=MESH,
        )

    patch_part, sub_part = pl.ds(0, 2 * sent), pl.ds(2 * sent, 2 * sent)

    def listen(slot, pieces):
        for j in pieces:
            arrival(slot, j).wait_recv()
            high, low = halves(heard_ref[slot, j])
            heard_pair[pl.ds(j * sent, sent), :columns] = high
            heard_pair[pl.ds(j * sent, sent), columns:] = low

    def far_product(at, part):
        return product(far_hi[at, part], far_lo[at, part], heard_pair[part], columns)

    def step(slot, damping, last, heard):
        at = own if last else pl.ds(0, packed_rows + rows)
        total_ref[at] = product(near_hi[at], near_lo[at], pair_ref[...], columns)
        if heard:
            listen(slot, (2, 3))
        total_ref[at] = total_ref[at] + far_product(at, sub_part)
        if heard:
            listen(slot, (0, 1))
        if last:
            residual_ref[...] = residual_ref[...] - (total_ref[own] + far_product(own, patch_part))
            return damping
        damping_next = 1.0 / (2.0 * ratio - damping)
        keep = damping_next * damping
        gain = 2.0 * damping_next / half_width
        for group in (0, 2):
            span = pl.ds(group * sent, 2 * sent)
            update = total_ref[span] + far_product(span, patch_part)
            rest = packed_residual[span] - update
            packed_residual[span] = rest
            for i in range(2):
                j = group + i
                packed_ref[slot + 1, j] = (
                    keep * packed_ref[slot, j] + gain * rest[i * sent : (i + 1) * sent]
                )
                exchange(slot + 1, j).start()
        residual = residual_ref[...] - (total_ref[own] + far_product(own, patch_part))
        residual_ref[...] = residual
        direction = keep * direction_ref[...] + gain * residual
        direction_ref[...] = direction
        solution_ref[...] = solution_ref[...] + direction
        high, low = halves(direction)
        pair_ref[:, :columns] = high
        pair_ref[:, columns:] = low
        return damping_next

    damping = step(0, 1.0 / ratio, False, False)
    damping = lax.fori_loop(1, ITERS - 1, lambda k, d: step(k, d, False, True), damping)
    step(ITERS - 1, damping, True, True)

    final = residual_ref[...]
    norms_ref[me] = jnp.sum(final * final, axis=0, keepdims=True)

    @pl.loop(1, devices)
    def _(step):
        other = lax.rem(me + step, devices)
        pltpu.make_async_remote_copy(
            src_ref=norms_ref.at[me], dst_ref=norms_ref.at[me],
            send_sem=norm_send, recv_sem=norm_recv,
            device_id=(other // n_sub, lax.rem(other, n_sub)), device_id_type=MESH,
        ).start()

    for slot in range(1, ITERS):
        for j in range(4):
            exchange(slot, j).wait_send()
    others = norms_ref.at[pl.ds(0, devices - 1)]
    pltpu.make_async_copy(others, others, norm_recv).wait()
    pltpu.make_async_copy(others, others, norm_send).wait()
    norm_ref[...] = jnp.sqrt(jnp.sum(norms_ref[...], axis=0))


def solution(mesh):
    n_patch, n_sub = mesh.shape["patch"], mesh.shape["sub"]

    def on_device(sources, diag_coef, tiles, tile_cols, send_rows, recv_rows, bounds):
        blk_rows, per_row, size, _ = tiles.shape
        rows = diag_coef.shape[0]
        columns = sources.shape[0]
        sent = send_rows.shape[2]
        halo = recv_rows.shape[1]
        every = 4 * sent + rows
        vmem, smem = pltpu.VMEM, pltpu.SMEM
        result, norm = pl.pallas_call(
            functools.partial(kernel, n_patch, n_sub),
            out_shape=(
                jax.ShapeDtypeStruct((rows, columns), F32),
                jax.ShapeDtypeStruct((1, columns), F32),
            ),
            in_specs=[
                pl.BlockSpec(memory_space=vmem),
                pl.BlockSpec(memory_space=vmem),
                pl.BlockSpec(memory_space=pl.ANY),
                pl.BlockSpec(memory_space=smem),
                pl.BlockSpec(memory_space=vmem),
                pl.BlockSpec(memory_space=vmem),
                pl.BlockSpec(memory_space=smem),
            ],
            out_specs=(pl.BlockSpec(memory_space=vmem), pl.BlockSpec(memory_space=vmem)),
            scratch_shapes=[
                vmem(tiles.shape, F32),
                vmem((every, rows), BF16),
                vmem((every, rows), BF16),
                vmem((every, halo), BF16),
                vmem((every, halo), BF16),
                vmem((rows, halo), BF16),
                vmem((rows, halo), BF16),
                vmem((rows, columns), F32),
                vmem((rows, columns), F32),
                vmem((4 * sent, columns), F32),
                vmem((every, columns), F32),
                vmem((rows, 2 * columns), BF16),
                vmem((4 * sent, 2 * columns), BF16),
                vmem((ITERS, 4, sent, columns), F32),
                vmem((ITERS, 4, sent, columns), F32),
                vmem((4, 1, sent), jnp.int32),
                vmem((n_patch * n_sub, 1, columns), F32),
                pltpu.SemaphoreType.DMA((blk_rows,)),
                pltpu.SemaphoreType.DMA((4,)),
                pltpu.SemaphoreType.DMA((4,)),
                pltpu.SemaphoreType.DMA((ITERS, 4)),
                pltpu.SemaphoreType.DMA((ITERS, 4)),
                pltpu.SemaphoreType.DMA,
                pltpu.SemaphoreType.DMA,
            ],
            compiler_params=pltpu.CompilerParams(collective_id=0, has_side_effects=True),
            name="chebyshev",
        )(
            sources.T,
            diag_coef.reshape(blk_rows, size),
            tiles,
            tile_cols,
            send_rows.reshape(4, 1, sent),
            recv_rows,
            bounds,
        )
        return result, norm.reshape(columns)

    return jax.shard_map(
        on_device,
        mesh=mesh,
        in_specs=(
            P(),
            P(("patch", "sub")),
            P(("patch", "sub"), None, None, None),
            P(("patch", "sub"), None),
            P(("patch", "sub"), None, None),
            P(("patch", "sub"), None),
            P(),
        ),
        out_specs=(P(("patch", "sub"), None), P()),
        check_vma=False,
    )
```

```python
import functools

import jax
import jax.numpy as jnp
from jax import lax
from jax.experimental import pallas as pl
from jax.experimental.pallas import tpu as pltpu
from jax.sharding import PartitionSpec as P

ITERS = 8
MESH = pl.DeviceIdType.MESH
F32 = jnp.float32
BF16 = jnp.bfloat16


def halves(value):
    high = value.astype(BF16)
    return high, (value - high.astype(F32)).astype(BF16)


def product(high, low, pair, columns):
    wide = jnp.dot(high, pair, preferred_element_type=F32)
    narrow = jnp.dot(low, pair[:, :columns], preferred_element_type=F32)
    return wide[:, :columns] + wide[:, columns:] + narrow


def kernel(
    n_patch, n_sub,
    sources_ref, diag_ref, tiles_hbm, cols_ref, sends_ref, receives_ref, bounds_ref,
    solution_ref, norm_ref,
    tiles_ref, near_hi, near_lo, far_hi, far_lo, halo_hi, halo_lo,
    direction_ref, residual_ref, packed_residual, total_ref, pair_ref, heard_pair,
    packed_ref, heard_ref, heard_rows, norms_ref, counts_ref, pick_ref, place_ref,
    tile_sems, row_send, row_recv, send_sems, recv_sems, norm_send, norm_recv,
):
    blk_rows, per_row, size, _ = tiles_hbm.shape
    rows = blk_rows * size
    n_src, columns = sources_ref.shape
    sent = sends_ref.shape[2]
    halo = receives_ref.shape[1]
    packed_rows = 4 * sent
    patch, sub = lax.axis_index("patch"), lax.axis_index("sub")
    devices = n_patch * n_sub
    me = patch * n_sub + sub

    copies = [
        pltpu.make_async_copy(tiles_hbm.at[b], tiles_ref.at[b], tile_sems.at[b])
        for b in range(blk_rows)
    ]
    for copy in copies:
        copy.start()

    barrier = pltpu.get_barrier_semaphore()

    @pl.loop(1, devices)
    def _(step):
        other = lax.rem(me + step, devices)
        pl.semaphore_signal(
            barrier, inc=1, device_id=(other // n_sub, lax.rem(other, n_sub)), device_id_type=MESH
        )

    lower_patch = lax.rem(patch + n_patch - 1, n_patch)
    upper_patch = lax.rem(patch + 1, n_patch)
    lower_sub = lax.rem(sub + n_sub - 1, n_sub)
    upper_sub = lax.rem(sub + 1, n_sub)
    targets = [(lower_patch, sub), (upper_patch, sub), (patch, lower_sub), (patch, upper_sub)]
    lands = [1, 0, 3, 2]
    origins = [targets[0], targets[1], targets[2], targets[3]]

    low_end = jnp.full((1, columns), bounds_ref[0], F32)
    high_end = jnp.full((1, columns), bounds_ref[1], F32)
    centre = (low_end + high_end) / 2.0
    half_width = (high_end - low_end) / 2.0
    ratio = centre / half_width

    def counted(ids):
        total = jnp.zeros(ids.shape, F32)
        for s in range(n_src):
            total = total + jnp.where(sources_ref[s : s + 1, :] == ids, 1.0, 0.0)
        return total

    right_side = counted(me * rows + lax.broadcasted_iota(jnp.int32, (rows, columns), 0))
    counts_ref[...] = right_side

    def as_column(row, width):
        return jnp.broadcast_to(row, (width, row.shape[1])).T

    picks = []
    for j in range(4):
        wide = as_column(sends_ref[j], rows)
        picks.append(
            jnp.where(wide == lax.broadcasted_iota(jnp.int32, (sent, rows), 1), 1.0, 0.0).astype(BF16)
        )
    pick_ref[...] = jnp.concatenate(picks, axis=0)
    for i in range(halo // size):
        wide = as_column(receives_ref[:, i * size : (i + 1) * size], packed_rows)
        place_ref[pl.ds(i * size, size)] = jnp.where(
            wide == lax.broadcasted_iota(jnp.int32, (size, packed_rows), 1), 1.0, 0.0
        ).astype(BF16)

    pl.semaphore_wait(barrier, devices - 1)
    row_copies = []
    for j in range(4):
        copy = pltpu.make_async_remote_copy(
            src_ref=sends_ref.at[j], dst_ref=heard_rows.at[lands[j]],
            send_sem=row_send.at[j], recv_sem=row_recv.at[lands[j]],
            device_id=targets[j], device_id_type=MESH,
        )
        copy.start()
        row_copies.append(copy)

    eye = lax.broadcasted_iota(jnp.int32, (size, size), 0) == lax.broadcasted_iota(
        jnp.int32, (size, size), 1
    )
    for b in range(blk_rows):
        copies[b].wait()
        for c in range(blk_rows + halo // size):
            block = jnp.zeros((size, size), F32)
            for n in range(per_row):
                block = block + tiles_ref[b, n] * (cols_ref[b, n] == c).astype(F32)
            if c == b:
                block = block + jnp.where(eye, diag_ref[b : b + 1, :], 0.0)
            high, low = halves(block)
            at = pl.ds(packed_rows + b * size, size)
            if c < blk_rows:
                near_hi[at, pl.ds(c * size, size)] = high
                near_lo[at, pl.ds(c * size, size)] = low
            else:
                place_at = pl.ds((c - blk_rows) * size, size)
                halo_hi[pl.ds(b * size, size), place_at] = high
                halo_lo[pl.ds(b * size, size), place_at] = low
    own = pl.ds(packed_rows, rows)
    first = pl.ds(0, packed_rows)

    heard_counts = []
    for j in range(4):
        row_copies[j].wait()
    for j in range(4):
        base = (origins[j][0] * n_sub + origins[j][1]) * rows
        heard_counts.append(counted(base + as_column(heard_rows[j], columns)).astype(BF16))
    halo_counts = jnp.dot(
        place_ref[...], jnp.concatenate(heard_counts, axis=0), preferred_element_type=F32
    ).astype(BF16)

    def exchange(slot, j):
        return pltpu.make_async_remote_copy(
            src_ref=packed_ref.at[slot, j], dst_ref=heard_ref.at[slot, lands[j]],
            send_sem=send_sems.at[slot, j], recv_sem=recv_sems.at[slot, lands[j]],
            device_id=targets[j], device_id_type=MESH,
        )

    def arrival(slot, j):
        return pltpu.make_async_remote_copy(
            src_ref=packed_ref.at[slot, j], dst_ref=heard_ref.at[slot, j],
            send_sem=send_sems.at[slot, j], recv_sem=recv_sems.at[slot, j],
            device_id=targets[j], device_id_type=MESH,
        )

    patch_part, sub_part = pl.ds(0, 2 * sent), pl.ds(2 * sent, 2 * sent)

    def listen(slot, pieces):
        for j in pieces:
            arrival(slot, j).wait_recv()
            high, low = halves(heard_ref[slot, j])
            heard_pair[pl.ds(j * sent, sent), :columns] = high
            heard_pair[pl.ds(j * sent, sent), columns:] = low

    def far_product(at, part):
        return product(far_hi[at, part], far_lo[at, part], heard_pair[part], columns)

    def advance(damping):
        damping_next = 1.0 / (2.0 * ratio - damping)
        return damping_next, damping_next * damping, 2.0 * damping_next / half_width

    def step(slot, damping, last):
        at = own if last else pl.ds(0, packed_rows + rows)
        total_ref[at] = product(near_hi[at], near_lo[at], pair_ref[...], columns)
        listen(slot, (2, 3))
        total_ref[at] = total_ref[at] + far_product(at, sub_part)
        listen(slot, (0, 1))
        if last:
            residual_ref[...] = residual_ref[...] - (total_ref[own] + far_product(own, patch_part))
            return damping
        damping_next, keep, gain = advance(damping)
        for group in (0, 2):
            span = pl.ds(group * sent, 2 * sent)
            update = total_ref[span] + far_product(span, patch_part)
            rest = packed_residual[span] - update
            packed_residual[span] = rest
            for i in range(2):
                j = group + i
                packed_ref[slot + 1, j] = (
                    keep * packed_ref[slot, j] + gain * rest[i * sent : (i + 1) * sent]
                )
                exchange(slot + 1, j).start()
        residual = residual_ref[...] - (total_ref[own] + far_product(own, patch_part))
        residual_ref[...] = residual
        direction = keep * direction_ref[...] + gain * residual
        direction_ref[...] = direction
        solution_ref[...] = solution_ref[...] + direction
        high, low = halves(direction)
        pair_ref[:, :columns] = high
        pair_ref[:, columns:] = low
        return damping_next

    counts = counts_ref[...].astype(BF16)
    product_sum = (
        jnp.dot(near_hi[own], counts, preferred_element_type=F32)
        + jnp.dot(near_lo[own], counts, preferred_element_type=F32)
        + jnp.dot(halo_hi[...], halo_counts, preferred_element_type=F32)
        + jnp.dot(halo_lo[...], halo_counts, preferred_element_type=F32)
    )
    right_side = counts_ref[...]
    residual = right_side - product_sum / centre
    damping, keep, gain = advance(1.0 / ratio)
    before = right_side / centre
    direction = keep * before + gain * residual
    high, low = halves(direction)
    pair_ref[:, :columns] = high
    pair_ref[:, columns:] = low
    for group in (0, 2):
        wide = jnp.dot(
            pick_ref[pl.ds(group * sent, 2 * sent)], pair_ref[...], preferred_element_type=F32
        )
        wide = wide[:, :columns] + wide[:, columns:]
        for i in range(2):
            packed_ref[1, group + i] = wide[i * sent : (i + 1) * sent]
            exchange(1, group + i).start()
    residual_ref[...] = residual
    direction_ref[...] = direction
    solution_ref[...] = before + direction
    high, low = halves(residual)
    wide = jnp.dot(pick_ref[...], jnp.concatenate([high, low], axis=1), preferred_element_type=F32)
    packed_residual[...] = wide[:, :columns] + wide[:, columns:]

    for halo_part, far, near in ((halo_hi, far_hi, near_hi), (halo_lo, far_lo, near_lo)):
        far[own] = jnp.dot(
            halo_part[...], place_ref[...], preferred_element_type=F32
        ).astype(BF16)
        far[first] = jnp.dot(pick_ref[...], far[own], preferred_element_type=F32).astype(BF16)
        near[first] = jnp.dot(pick_ref[...], near[own], preferred_element_type=F32).astype(BF16)

    damping = lax.fori_loop(1, ITERS - 1, lambda k, d: step(k, d, False), damping)
    step(ITERS - 1, damping, True)

    final = residual_ref[...]
    norms_ref[me] = jnp.sum(final * final, axis=0, keepdims=True)

    @pl.loop(1, devices)
    def _(step):
        other = lax.rem(me + step, devices)
        pltpu.make_async_remote_copy(
            src_ref=norms_ref.at[me], dst_ref=norms_ref.at[me],
            send_sem=norm_send, recv_sem=norm_recv,
            device_id=(other // n_sub, lax.rem(other, n_sub)), device_id_type=MESH,
        ).start()

    for slot in range(1, ITERS):
        for j in range(4):
            exchange(slot, j).wait_send()
    others = norms_ref.at[pl.ds(0, devices - 1)]
    pltpu.make_async_copy(others, others, norm_recv).wait()
    pltpu.make_async_copy(others, others, norm_send).wait()
    norm_ref[...] = norms_ref[...]


def finish(solution_ref, norms_ref, result_ref, norm_ref):
    result_ref[...] = solution_ref[...]
    norm_ref[...] = jnp.sqrt(jnp.sum(norms_ref[...], axis=0))


def solution(mesh):
    n_patch, n_sub = mesh.shape["patch"], mesh.shape["sub"]

    def on_device(sources, diag_coef, tiles, tile_cols, send_rows, recv_rows, bounds):
        blk_rows, per_row, size, _ = tiles.shape
        rows = diag_coef.shape[0]
        columns = sources.shape[0]
        sent = send_rows.shape[2]
        halo = recv_rows.shape[1]
        every = 4 * sent + rows
        vmem, smem = pltpu.VMEM, pltpu.SMEM
        held, norms = pl.pallas_call(
            functools.partial(kernel, n_patch, n_sub),
            out_shape=(
                jax.ShapeDtypeStruct((rows, columns), F32),
                jax.ShapeDtypeStruct((n_patch * n_sub, 1, columns), F32),
            ),
            in_specs=[
                pl.BlockSpec(memory_space=vmem),
                pl.BlockSpec(memory_space=vmem),
                pl.BlockSpec(memory_space=pl.ANY),
                pl.BlockSpec(memory_space=smem),
                pl.BlockSpec(memory_space=vmem),
                pl.BlockSpec(memory_space=vmem),
                pl.BlockSpec(memory_space=smem),
            ],
            out_specs=(pl.BlockSpec(memory_space=vmem), pl.BlockSpec(memory_space=vmem)),
            scratch_shapes=[
                vmem(tiles.shape, F32),
                vmem((every, rows), BF16),
                vmem((every, rows), BF16),
                vmem((every, halo), BF16),
                vmem((every, halo), BF16),
                vmem((rows, halo), BF16),
                vmem((rows, halo), BF16),
                vmem((rows, columns), F32),
                vmem((rows, columns), F32),
                vmem((4 * sent, columns), F32),
                vmem((every, columns), F32),
                vmem((rows, 2 * columns), BF16),
                vmem((4 * sent, 2 * columns), BF16),
                vmem((ITERS, 4, sent, columns), F32),
                vmem((ITERS, 4, sent, columns), F32),
                vmem((4, 1, sent), jnp.int32),
                vmem((n_patch * n_sub, 1, columns), F32),
                vmem((rows, columns), F32),
                vmem((4 * sent, rows), BF16),
                vmem((halo, 4 * sent), BF16),
                pltpu.SemaphoreType.DMA((blk_rows,)),
                pltpu.SemaphoreType.DMA((4,)),
                pltpu.SemaphoreType.DMA((4,)),
                pltpu.SemaphoreType.DMA((ITERS, 4)),
                pltpu.SemaphoreType.DMA((ITERS, 4)),
                pltpu.SemaphoreType.DMA,
                pltpu.SemaphoreType.DMA,
            ],
            compiler_params=pltpu.CompilerParams(collective_id=0, has_side_effects=True),
            name="chebyshev",
        )(
            sources.T,
            diag_coef.reshape(blk_rows, size),
            tiles,
            tile_cols,
            send_rows.reshape(4, 1, sent),
            recv_rows,
            bounds,
        )
        result, norm = pl.pallas_call(
            finish,
            out_shape=(
                jax.ShapeDtypeStruct((rows, columns), F32),
                jax.ShapeDtypeStruct((1, columns), F32),
            ),
            in_specs=[pl.BlockSpec(memory_space=vmem)] * 2,
            out_specs=(pl.BlockSpec(memory_space=vmem), pl.BlockSpec(memory_space=vmem)),
            name="finish",
        )(held, norms)
        return result, norm.reshape(columns)

    return jax.shard_map(
        on_device,
        mesh=mesh,
        in_specs=(
            P(),
            P(("patch", "sub")),
            P(("patch", "sub"), None, None, None),
            P(("patch", "sub"), None),
            P(("patch", "sub"), None, None),
            P(("patch", "sub"), None),
            P(),
        ),
        out_specs=(P(("patch", "sub"), None), P()),
        check_vma=False,
    )
```

```python
import functools

import jax
import jax.numpy as jnp
from jax import lax
from jax.experimental import pallas as pl
from jax.experimental.pallas import tpu as pltpu
from jax.sharding import PartitionSpec as P

ITERS = 8
MESH = pl.DeviceIdType.MESH
F32 = jnp.float32
BF16 = jnp.bfloat16


def halves(value):
    high = value.astype(BF16)
    return high, (value - high.astype(F32)).astype(BF16)


def product(high, low, pair, columns):
    wide = jnp.dot(high, pair, preferred_element_type=F32)
    narrow = jnp.dot(low, pair[:, :columns], preferred_element_type=F32)
    return wide[:, :columns] + wide[:, columns:] + narrow


def kernel(
    n_patch, n_sub,
    sources_ref, diag_ref, tiles_hbm, cols_ref, sends_ref, receives_ref, bounds_ref,
    solution_ref, norm_ref,
    tiles_ref, near_hi, near_lo, far_hi, far_lo, halo_hi, halo_lo,
    direction_ref, residual_ref, packed_residual, total_ref, pair_ref, heard_pair,
    packed_ref, heard_ref, heard_rows, norms_ref, counts_ref, pick_ref, place_ref,
    message_ref, echo_out, echo_in, echo_hi, echo_lo, echo_sems,
    tile_sems, row_send, row_recv, send_sems, recv_sems, norm_send, norm_recv,
):
    blk_rows, per_row, size, _ = tiles_hbm.shape
    rows = blk_rows * size
    n_src, columns = sources_ref.shape
    sent = sends_ref.shape[2]
    halo = receives_ref.shape[1]
    packed_rows = 4 * sent
    patch, sub = lax.axis_index("patch"), lax.axis_index("sub")
    devices = n_patch * n_sub
    me = patch * n_sub + sub

    copies = [
        pltpu.make_async_copy(tiles_hbm.at[b], tiles_ref.at[b], tile_sems.at[b])
        for b in range(blk_rows)
    ]
    for copy in copies:
        copy.start()

    barrier = pltpu.get_barrier_semaphore()

    @pl.loop(1, devices)
    def _(step):
        other = lax.rem(me + step, devices)
        pl.semaphore_signal(
            barrier, inc=1, device_id=(other // n_sub, lax.rem(other, n_sub)), device_id_type=MESH
        )

    lower_patch = lax.rem(patch + n_patch - 1, n_patch)
    upper_patch = lax.rem(patch + 1, n_patch)
    lower_sub = lax.rem(sub + n_sub - 1, n_sub)
    upper_sub = lax.rem(sub + 1, n_sub)
    targets = [(lower_patch, sub), (upper_patch, sub), (patch, lower_sub), (patch, upper_sub)]
    lands = [1, 0, 3, 2]
    origins = [targets[0], targets[1], targets[2], targets[3]]

    low_end = jnp.full((1, columns), bounds_ref[0], F32)
    high_end = jnp.full((1, columns), bounds_ref[1], F32)
    centre = (low_end + high_end) / 2.0
    half_width = (high_end - low_end) / 2.0
    ratio = centre / half_width

    def counted(ids):
        total = jnp.zeros(ids.shape, F32)
        for s in range(n_src):
            total = total + jnp.where(sources_ref[s : s + 1, :] == ids, 1.0, 0.0)
        return total

    right_side = counted(me * rows + lax.broadcasted_iota(jnp.int32, (rows, columns), 0))
    counts_ref[...] = right_side

    def as_column(row, width):
        return jnp.broadcast_to(row, (width, row.shape[1])).T

    picks = []
    for j in range(4):
        wide = as_column(sends_ref[j], rows)
        picks.append(
            jnp.where(wide == lax.broadcasted_iota(jnp.int32, (sent, rows), 1), 1.0, 0.0).astype(BF16)
        )
    pick_ref[...] = jnp.concatenate(picks, axis=0)
    for i in range(halo // size):
        wide = as_column(receives_ref[:, i * size : (i + 1) * size], packed_rows)
        place_ref[pl.ds(i * size, size)] = jnp.where(
            wide == lax.broadcasted_iota(jnp.int32, (size, packed_rows), 1), 1.0, 0.0
        ).astype(BF16)

    pl.semaphore_wait(barrier, devices - 1)
    row_copies = []
    for j in range(4):
        copy = pltpu.make_async_remote_copy(
            src_ref=sends_ref.at[j], dst_ref=heard_rows.at[lands[j]],
            send_sem=row_send.at[j], recv_sem=row_recv.at[lands[j]],
            device_id=targets[j], device_id_type=MESH,
        )
        copy.start()
        row_copies.append(copy)

    eye = lax.broadcasted_iota(jnp.int32, (size, size), 0) == lax.broadcasted_iota(
        jnp.int32, (size, size), 1
    )
    for b in range(blk_rows):
        copies[b].wait()
        for c in range(blk_rows + halo // size):
            block = jnp.zeros((size, size), F32)
            for n in range(per_row):
                block = block + tiles_ref[b, n] * (cols_ref[b, n] == c).astype(F32)
            if c == b:
                block = block + jnp.where(eye, diag_ref[b : b + 1, :], 0.0)
            high, low = halves(block)
            at = pl.ds(packed_rows + b * size, size)
            if c < blk_rows:
                near_hi[at, pl.ds(c * size, size)] = high
                near_lo[at, pl.ds(c * size, size)] = low
            else:
                place_at = pl.ds((c - blk_rows) * size, size)
                halo_hi[pl.ds(b * size, size), place_at] = high
                halo_lo[pl.ds(b * size, size), place_at] = low
    own = pl.ds(packed_rows, rows)
    first = pl.ds(0, packed_rows)

    heard_counts = []
    for j in range(4):
        row_copies[j].wait()
    for j in range(4):
        base = (origins[j][0] * n_sub + origins[j][1]) * rows
        heard_counts.append(counted(base + as_column(heard_rows[j], columns)).astype(BF16))
    halo_counts = jnp.dot(
        place_ref[...], jnp.concatenate(heard_counts, axis=0), preferred_element_type=F32
    ).astype(BF16)

    def exchange(slot, j):
        return pltpu.make_async_remote_copy(
            src_ref=packed_ref.at[slot, j], dst_ref=heard_ref.at[slot, lands[j]],
            send_sem=send_sems.at[slot, j], recv_sem=recv_sems.at[slot, lands[j]],
            device_id=targets[j], device_id_type=MESH,
        )

    def arrival(slot, j):
        return pltpu.make_async_remote_copy(
            src_ref=packed_ref.at[slot, j], dst_ref=heard_ref.at[slot, j],
            send_sem=send_sems.at[slot, j], recv_sem=recv_sems.at[slot, j],
            device_id=targets[0], device_id_type=MESH,
        )

    patch_part, sub_part = pl.ds(0, 2 * sent), pl.ds(2 * sent, 2 * sent)

    def listen(slot, pieces):
        for j in pieces:
            arrival(slot, j).wait_recv()
            high, low = halves(heard_ref[slot, j])
            heard_pair[pl.ds(j * sent, sent), :columns] = high
            heard_pair[pl.ds(j * sent, sent), columns:] = low

    def far_product(at, part):
        return product(far_hi[at, part], far_lo[at, part], heard_pair[part], columns)

    def advance(damping):
        damping_next = 1.0 / (2.0 * ratio - damping)
        return damping_next, damping_next * damping, 2.0 * damping_next / half_width

    distant = lax.rem(patch, 2)
    close = 1 - distant
    distant_part = pl.ds(pl.multiple_of(distant * sent, sent), sent)
    close_part = pl.ds(pl.multiple_of(close * sent, sent), sent)

    def patch_copy(source, slot, j):
        return pltpu.make_async_remote_copy(
            src_ref=source, dst_ref=heard_ref.at[slot, 1 - j],
            send_sem=send_sems.at[slot, j], recv_sem=recv_sems.at[slot, 1 - j],
            device_id=(lax.rem(patch + n_patch + 2 * j - 1, n_patch), sub), device_id_type=MESH,
        )

    def step(slot, damping, gain_before, last):
        at = own if last else pl.ds(0, packed_rows + rows)
        total_ref[at] = product(near_hi[at], near_lo[at], pair_ref[...], columns)
        high, low = halves(packed_ref[slot - 1, distant])
        echo = gain_before * product(
            echo_hi[...], echo_lo[...], jnp.concatenate([high, low], axis=1), columns
        )
        listen(slot, (2, 3))
        total_ref[at] = total_ref[at] + far_product(at, sub_part)
        arrival(slot, close).wait_recv()
        high, low = halves(heard_ref[slot, close])
        heard_pair[close_part, :columns] = high
        heard_pair[close_part, columns:] = low
        if not last:
            damping_next, keep, gain = advance(damping)
            total = total_ref[distant_part] + far_product(distant_part, close_part)
            message_ref[slot + 1] = keep * packed_ref[slot, distant] + gain * (
                packed_residual[distant_part] - total
            )
            patch_copy(message_ref.at[slot + 1], slot + 1, distant).start()
        arrival(slot, distant).wait_recv()
        high, low = halves(heard_ref[slot, distant] - echo)
        heard_pair[distant_part, :columns] = high
        heard_pair[distant_part, columns:] = low
        if last:
            residual_ref[...] = residual_ref[...] - (total_ref[own] + far_product(own, patch_part))
            return
        for group in (0, 2):
            span = pl.ds(group * sent, 2 * sent)
            rest = packed_residual[span] - (total_ref[span] + far_product(span, patch_part))
            packed_residual[span] = rest
            for i in range(2):
                packed_ref[slot + 1, group + i] = (
                    keep * packed_ref[slot, group + i] + gain * rest[i * sent : (i + 1) * sent]
                )
            if group == 0:
                patch_copy(packed_ref.at[slot + 1, close], slot + 1, close).start()
            else:
                exchange(slot + 1, 2).start()
                exchange(slot + 1, 3).start()
        residual = residual_ref[...] - (total_ref[own] + far_product(own, patch_part))
        residual_ref[...] = residual
        direction = keep * direction_ref[...] + gain * residual
        direction_ref[...] = direction
        solution_ref[...] = solution_ref[...] + direction
        high, low = halves(direction)
        pair_ref[:, :columns] = high
        pair_ref[:, columns:] = low
        return damping_next, gain

    counts = counts_ref[...].astype(BF16)
    product_sum = (
        jnp.dot(near_hi[own], counts, preferred_element_type=F32)
        + jnp.dot(near_lo[own], counts, preferred_element_type=F32)
        + jnp.dot(halo_hi[...], halo_counts, preferred_element_type=F32)
        + jnp.dot(halo_lo[...], halo_counts, preferred_element_type=F32)
    )
    right_side = counts_ref[...]
    residual = right_side - product_sum / centre
    damping, keep, gain = advance(1.0 / ratio)
    before = right_side / centre
    direction = keep * before + gain * residual
    high, low = halves(direction)
    pair_ref[:, :columns] = high
    pair_ref[:, columns:] = low
    for group in (0, 2):
        wide = jnp.dot(
            pick_ref[pl.ds(group * sent, 2 * sent)], pair_ref[...], preferred_element_type=F32
        )
        wide = wide[:, :columns] + wide[:, columns:]
        for i in range(2):
            packed_ref[1, group + i] = wide[i * sent : (i + 1) * sent]
            exchange(1, group + i).start()
    residual_ref[...] = residual
    direction_ref[...] = direction
    solution_ref[...] = before + direction
    high, low = halves(residual)
    wide = jnp.dot(pick_ref[...], jnp.concatenate([high, low], axis=1), preferred_element_type=F32)
    packed_residual[...] = wide[:, :columns] + wide[:, columns:]

    for halo_part, far, near in ((halo_hi, far_hi, near_hi), (halo_lo, far_lo, near_lo)):
        far[own] = jnp.dot(
            halo_part[...], place_ref[...], preferred_element_type=F32
        ).astype(BF16)
        far[first] = jnp.dot(pick_ref[...], far[own], preferred_element_type=F32).astype(BF16)
        near[first] = jnp.dot(pick_ref[...], near[own], preferred_element_type=F32).astype(BF16)

    echo_out[...] = far_hi[distant_part, distant_part].astype(F32) + far_lo[
        distant_part, distant_part
    ].astype(F32)
    echo_copy = pltpu.make_async_remote_copy(
        src_ref=echo_out, dst_ref=echo_in, send_sem=echo_sems.at[0], recv_sem=echo_sems.at[1],
        device_id=(lax.rem(patch + n_patch + 2 * distant - 1, n_patch), sub), device_id_type=MESH,
    )
    echo_copy.start()
    for j in range(2):
        packed_ref[0, j] = jnp.zeros((sent, columns), F32)
    echo_hi[...] = jnp.zeros((sent, sent), BF16)
    echo_lo[...] = jnp.zeros((sent, sent), BF16)
    state = step(1, damping, jnp.zeros((1, columns), F32), False)
    echo_copy.wait()
    echo_hi[...], echo_lo[...] = halves(echo_in[...])
    damping, gain = lax.fori_loop(2, ITERS - 1, lambda k, state: step(k, *state, False), state)
    step(ITERS - 1, damping, gain, True)

    final = residual_ref[...]
    norms_ref[me] = jnp.sum(final * final, axis=0, keepdims=True)

    @pl.loop(1, devices)
    def _(step):
        other = lax.rem(me + step, devices)
        pltpu.make_async_remote_copy(
            src_ref=norms_ref.at[me], dst_ref=norms_ref.at[me],
            send_sem=norm_send, recv_sem=norm_recv,
            device_id=(other // n_sub, lax.rem(other, n_sub)), device_id_type=MESH,
        ).start()

    for slot in range(1, ITERS):
        for j in range(4):
            exchange(slot, j).wait_send()
    others = norms_ref.at[pl.ds(0, devices - 1)]
    pltpu.make_async_copy(others, others, norm_recv).wait()
    pltpu.make_async_copy(others, others, norm_send).wait()
    norm_ref[...] = norms_ref[...]


def finish(solution_ref, norms_ref, result_ref, norm_ref):
    result_ref[...] = solution_ref[...]
    norm_ref[...] = jnp.sqrt(jnp.sum(norms_ref[...], axis=0))


def solution(mesh):
    n_patch, n_sub = mesh.shape["patch"], mesh.shape["sub"]

    def on_device(sources, diag_coef, tiles, tile_cols, send_rows, recv_rows, bounds):
        blk_rows, per_row, size, _ = tiles.shape
        rows = diag_coef.shape[0]
        columns = sources.shape[0]
        sent = send_rows.shape[2]
        halo = recv_rows.shape[1]
        every = 4 * sent + rows
        vmem, smem = pltpu.VMEM, pltpu.SMEM
        held, norms = pl.pallas_call(
            functools.partial(kernel, n_patch, n_sub),
            out_shape=(
                jax.ShapeDtypeStruct((rows, columns), F32),
                jax.ShapeDtypeStruct((n_patch * n_sub, 1, columns), F32),
            ),
            in_specs=[
                pl.BlockSpec(memory_space=vmem),
                pl.BlockSpec(memory_space=vmem),
                pl.BlockSpec(memory_space=pl.ANY),
                pl.BlockSpec(memory_space=smem),
                pl.BlockSpec(memory_space=vmem),
                pl.BlockSpec(memory_space=vmem),
                pl.BlockSpec(memory_space=smem),
            ],
            out_specs=(pl.BlockSpec(memory_space=vmem), pl.BlockSpec(memory_space=vmem)),
            scratch_shapes=[
                vmem(tiles.shape, F32),
                vmem((every, rows), BF16),
                vmem((every, rows), BF16),
                vmem((every, halo), BF16),
                vmem((every, halo), BF16),
                vmem((rows, halo), BF16),
                vmem((rows, halo), BF16),
                vmem((rows, columns), F32),
                vmem((rows, columns), F32),
                vmem((4 * sent, columns), F32),
                vmem((every, columns), F32),
                vmem((rows, 2 * columns), BF16),
                vmem((4 * sent, 2 * columns), BF16),
                vmem((ITERS, 4, sent, columns), F32),
                vmem((ITERS, 4, sent, columns), F32),
                vmem((4, 1, sent), jnp.int32),
                vmem((n_patch * n_sub, 1, columns), F32),
                vmem((rows, columns), F32),
                vmem((4 * sent, rows), BF16),
                vmem((halo, 4 * sent), BF16),
                vmem((ITERS, sent, columns), F32),
                vmem((sent, sent), F32),
                vmem((sent, sent), F32),
                vmem((sent, sent), BF16),
                vmem((sent, sent), BF16),
                pltpu.SemaphoreType.DMA((2,)),
                pltpu.SemaphoreType.DMA((blk_rows,)),
                pltpu.SemaphoreType.DMA((4,)),
                pltpu.SemaphoreType.DMA((4,)),
                pltpu.SemaphoreType.DMA((ITERS, 4)),
                pltpu.SemaphoreType.DMA((ITERS, 4)),
                pltpu.SemaphoreType.DMA,
                pltpu.SemaphoreType.DMA,
            ],
            compiler_params=pltpu.CompilerParams(collective_id=0, has_side_effects=True),
            name="chebyshev",
        )(
            sources.T,
            diag_coef.reshape(blk_rows, size),
            tiles,
            tile_cols,
            send_rows.reshape(4, 1, sent),
            recv_rows,
            bounds,
        )
        result, norm = pl.pallas_call(
            finish,
            out_shape=(
                jax.ShapeDtypeStruct((rows, columns), F32),
                jax.ShapeDtypeStruct((1, columns), F32),
            ),
            in_specs=[pl.BlockSpec(memory_space=vmem)] * 2,
            out_specs=(pl.BlockSpec(memory_space=vmem), pl.BlockSpec(memory_space=vmem)),
            name="finish",
        )(held, norms)
        return result, norm.reshape(columns)

    return jax.shard_map(
        on_device,
        mesh=mesh,
        in_specs=(
            P(),
            P(("patch", "sub")),
            P(("patch", "sub"), None, None, None),
            P(("patch", "sub"), None),
            P(("patch", "sub"), None, None),
            P(("patch", "sub"), None),
            P(),
        ),
        out_specs=(P(("patch", "sub"), None), P()),
        check_vma=False,
    )
```
